256 devices in a mesh: vx: 16 (over y, x), vy: 16 (over z, core).
Axes of the slice: x: 4, y: 4, z: 8, core: 2. Of those that a mesh axis runs over, the one named last changes fastest.
Arguments:
- hidden: bfloat16 [1024, 5120], P(('vx', 'vy')), may hold values from -96 to 96
- unembed: bfloat16 [152064, 5120], P(('vx', 'vy')), may hold values from -2 to 2
- loss_mask: int32 [1024], P(('vx', 'vy')), may hold values 0 or 1
- seq_ids: int32 [1024], P(('vx', 'vy')), may hold values from 0 to 7, never falling along the last dimension, each value on 1 to 256 neighbouring positions
Outputs:
- entropy: float32 [1024], P(('vx', 'vy'))
- seq_mean: float32 [8], replicated
The draws below stay inside these ranges and needn't reach their ends.
Inputs may be any that keep to these rules, and one draw needn't show every extreme that they name: `seq_ids`: sequence numbers never fall along the tokens; each sequence has 1 to 256 tokens.
All inputs are finite; a program needn't handle non-finite values. No bound on the sum of `loss_mask` on one device may be relied on, other than what follows from the above.
Results may differ from the reference program's by a relative error of at most 0.0013.
Values may be sent and summed in bfloat16 or wider, within the bound.
No kernel may reach another device: no remote copies, remote signals or barrier semaphores. Data moves between devices by JAX's collectives and lax.ppermute only.
A program may use at most 128 MiB of HBM per device.

```python
import math
import jax
import jax.numpy as jnp
import numpy as np
from jax import lax

D = 5120
VOCAB = 152064
SEQS = 8
TOKENS = 1024
SEG_MOST = 256
N_VX = 16
N_VY = 16


def unembed_rows(key, indices):

    def single(index):
        base = jax.random.normal(jax.random.fold_in(jax.random.fold_in(key, 11), index), (D,), jnp.float32) * D ** (-0.5)
        return base
    return jax.vmap(single)(indices)


def draw_unembed(key, part):
    rows = unembed_rows(key, jnp.arange(VOCAB, dtype=jnp.int32))
    return jnp.clip(rows, -2.0, 2.0).astype(jnp.bfloat16)


def draw_hidden(key, part):
    base = jax.random.normal(jax.random.fold_in(key, 21), (TOKENS, D), jnp.float32) * 4.0
    return jnp.clip(base, -96.0, 96.0).astype(jnp.bfloat16)


def place_ends(entries, key, smallest, largest):
    longest = entries.shape.index(max(entries.shape))
    spots = []
    for shift in (0, 1):
        where = [jax.random.randint(jax.random.fold_in(key, axis), (), 0, length) for axis, length in enumerate(entries.shape)]
        where[longest] = (where[longest] + shift) % entries.shape[longest]
        spots.append(tuple(where))
    return entries.at[spots[0]].set(smallest).at[spots[1]].set(largest)


def length_profile(count, total, limit, skew):
    weights = [(1 << 20) // math.isqrt(grade ** skew) + 1 for grade in range(2, count + 1)]
    rest, holding = total - limit - (count - 1), [1] * (count - 1)
    while rest > 0:
        free = [i for i in range(count - 1) if holding[i] < limit]
        whole, left = sum([weights[i] for i in free]), rest
        for i in free:
            addition = min(limit - holding[i], max(1, left * weights[i] // whole), rest)
            holding[i] = holding[i] + addition
            rest = rest - addition
    return np.array([limit] + holding)


def uneven(rng, amount, total, limit, slope):
    if amount == 2:
        one = jax.random.randint(rng, (), max(1, total - limit), min(limit, total - 1) + 1)
        return jnp.stack([one, total - one])
    lengths = jnp.asarray(length_profile(amount, total, limit, slope), jnp.int32)
    twos = (amount - 1) // 2
    donor, sink = lengths[1:1 + 2 * twos:2], lengths[2:2 + 2 * twos:2]
    margin = jnp.minimum(donor - 1, limit - sink)
    moved = jax.random.randint(jax.random.fold_in(rng, 1), (twos,), 0, 1 << 20) % (margin + 1)
    lengths = lengths.at[1:1 + 2 * twos:2].set(donor - moved).at[2:2 + 2 * twos:2].set(sink + moved)
    return lengths[jax.random.permutation(jax.random.fold_in(rng, 2), amount)]


def setup_inputs(seed: int = 0) -> dict:
    key_of = jax.random.split(jax.random.key(seed), 5)
    hidden = draw_hidden(jax.random.fold_in(key_of[4], 71), 0)
    unembed = draw_unembed(jax.random.fold_in(key_of[4], 71), 0)
    loss_mask = place_ends((jax.random.randint(key_of[2], (TOKENS,), 0, 4) < 3).astype(jnp.int32), jax.random.fold_in(key_of[2], 1), 0, 1)
    seq_ids = jnp.searchsorted(jnp.cumsum(uneven(key_of[3], SEQS, TOKENS, SEG_MOST, 1)), jnp.arange(TOKENS), side="right").astype(jnp.int32)
    return {"hidden": hidden, "unembed": unembed, "loss_mask": loss_mask, "seq_ids": seq_ids}


def combine_stats(earlier, later):
    joined = jnp.maximum(earlier[0], later[0])
    shift_a = earlier[0] - joined
    shift_b = later[0] - joined
    scale_a = jnp.exp(shift_a)
    scale_b = jnp.exp(shift_b)
    norms = scale_a * earlier[1] + scale_b * later[1]
    tilts = scale_a * (earlier[2] + shift_a * earlier[1]) + scale_b * (later[2] + shift_b * later[1])
    return (joined, norms, tilts)


def block_stats(hidden, block):
    logits = jnp.dot(hidden, block.T, preferred_element_type=jnp.float32)
    peaked = jnp.max(logits, axis=1)
    shifted = logits - peaked[:, None]
    expval = jnp.exp(shifted)
    return (peaked, jnp.sum(expval, axis=1), jnp.sum(expval * shifted, axis=1))


def reference(hidden, unembed, loss_mask, seq_ids):
    pieces = N_VX * N_VY
    span_size = VOCAB // pieces
    blocks = unembed.reshape(pieces, span_size, D)
    initial = block_stats(hidden, blocks[0])

    def advance(carry, block):
        return combine_stats(carry, block_stats(hidden, block)), None

    merged, unused = lax.scan(advance, initial, blocks[1:])
    entropy = jnp.log(merged[1]) - merged[2] / merged[1]
    member = (seq_ids[:, None] == jnp.arange(SEQS, dtype=jnp.int32)[None, :]) & (loss_mask[:, None] > 0)
    seq_sums = jnp.sum(entropy[:, None] * member.astype(jnp.float32), axis=0)
    seq_counts = jnp.sum(member.astype(jnp.int32), axis=0)
    seq_mean = seq_sums / jnp.maximum(seq_counts, 1).astype(jnp.float32)
    return entropy, seq_mean
```

```python
import jax
import jax.numpy as jnp
from jax import lax
from jax.sharding import Mesh
from jax.sharding import PartitionSpec as P

SEQS = 8
NY, NX, NZ, NC = 4, 4, 8, 2
ALL = ("y", "x", "z", "c")


def rank_of(y, x, z, c):
    return (((y % NY) * NX + x % NX) * NZ + z % NZ) * NC + c


def pairs(where):
    return [
        (rank_of(y, x, z, c), rank_of(*where(y, x, z, c)))
        for y in range(NY)
        for x in range(NX)
        for z in range(NZ)
        for c in range(NC)
    ]


def moved(value, where):
    return lax.ppermute(value, ALL, pairs(where))


def other_core(y, x, z, c):
    return (y, x, z, 1 - c)


def along_near(step):
    return lambda y, x, z, c: (y + step, x, z, c) if c == 0 else (y, x + step, z, c)


def along_far(step):
    return lambda y, x, z, c: (y, x + step, z, c) if c == 0 else (y + step, x, z, c)


def copy_for_each(shard, axis):
    copies = jnp.broadcast_to(shard, (lax.axis_size(axis), *shard.shape))
    return lax.all_to_all(copies, axis, split_axis=0, concat_axis=0, tiled=True)


def gathered(hidden):
    line = copy_for_each(hidden, "z").reshape(-1, hidden.shape[1])
    one = moved(line, along_near(-1))
    three = moved(line, along_near(1))
    two = moved(line, along_near(2))
    first = jnp.concatenate([line, one], axis=0)
    second = jnp.concatenate([two, three], axis=0)
    first_1 = moved(first, along_far(-1))
    second_3 = moved(second, along_far(1))
    second_1 = moved(second, along_far(-1))
    first_3 = moved(first, along_far(1))
    first_2 = moved(first_1, along_far(-1))
    second_2 = moved(second_3, along_far(1))
    return ((first, second), (first_1, second_1), (first_2, second_2), (first_3, second_3))


def block_stats(head, rows):
    logits = lax.dot_general(
        head, rows, (((1,), (1,)), ((), ())), preferred_element_type=jnp.float32
    )
    peak = jnp.max(logits, axis=0)
    shifted = logits - peak[None, :]
    weight = jnp.exp(shifted)
    return jnp.stack([peak, jnp.sum(weight, axis=0), jnp.sum(weight * shifted, axis=0)])


def joined(parts):
    peak = jnp.max(parts[:, 0], axis=0)
    shift = parts[:, 0] - peak[None]
    scale = jnp.exp(shift)
    norm = jnp.sum(scale * parts[:, 1], axis=0)
    tilt = jnp.sum(scale * (parts[:, 2] + shift * parts[:, 1]), axis=0)
    code = jnp.sum(parts[:, 3], axis=0)
    return jnp.stack([peak, norm, tilt, code])


def rolled(value, amount, axis):
    value = jnp.where(amount % 2 == 1, jnp.roll(value, 1, axis), value)
    return jnp.where(amount // 2 == 1, jnp.roll(value, 2, axis), value)


def per_device(hidden, unembed, loss_mask, seq_ids):
    y, x, z, c = (lax.axis_index(a) for a in ALL)
    near = jnp.where(c == 0, y, x)
    far = jnp.where(c == 0, x, y)
    head = jnp.concatenate([unembed, moved(unembed, other_core)], axis=0)
    groups = gathered(hidden)
    stats = [block_stats(head, jnp.concatenate(g, axis=0)) for g in groups]
    stats = jnp.stack(stats, axis=1).reshape(3, 4, 4, 32)
    stats = rolled(rolled(stats, far, 1), near, 2).reshape(3, 4, 128)
    own = jnp.where(loss_mask > 0, seq_ids + 1, 0).astype(jnp.float32)
    lane = lax.broadcasted_iota(jnp.int32, (4, 128), 1) // 4
    row = lax.broadcasted_iota(jnp.int32, (4, 128), 0)
    code = jnp.where((row == far) & (lane == near * NZ + z), jnp.tile(own, 32)[None, :], 0.0)
    mine = jnp.concatenate([stats, code[None]], axis=0)
    mine = joined(copy_for_each(mine, "z"))
    whole = joined(copy_for_each(mine, ("y", "x")))
    entropy_rows = jnp.log(whole[1]) - whole[2] / whole[1]
    flat, codes = entropy_rows.reshape(-1), whole[3].reshape(-1).astype(jnp.int32)
    entropy = lax.dynamic_slice_in_dim(flat, ((far * 4 + near) * NZ + z) * 4, 4)
    member = codes[None, :] == jnp.arange(1, SEQS + 1, dtype=jnp.int32)[:, None]
    sums = jnp.sum(jnp.where(member, flat[None, :], 0.0), axis=1)
    counts = jnp.sum(member.astype(jnp.float32), axis=1)
    both = jnp.stack([sums, counts])
    both = both + moved(both, other_core)
    seq_mean = both[0] / jnp.maximum(both[1], 1.0)
    return (entropy, seq_mean)


def solution(mesh):
    split = Mesh(mesh.devices.reshape(NY, NX, NZ, NC), ALL)
    return jax.shard_map(
        per_device,
        mesh=split,
        in_specs=(P(ALL, None), P(ALL, None), P(ALL), P(ALL)),
        out_specs=(P(ALL), P()),
        check_vma=False,
    )
```

```python
import functools

import jax
import jax.numpy as jnp
from jax import lax
from jax.experimental import pallas as pl
from jax.experimental.pallas import tpu as pltpu
from jax.sharding import Mesh
from jax.sharding import PartitionSpec as P


SEQS = 8
NY, NX, NZ, NC = 4, 4, 8, 2
ALL = ("y", "x", "z", "c")
LANES = 128
CHUNK = 600


def rank_of(y, x, z, c):
    return (((y % NY) * NX + x % NX) * NZ + z % NZ) * NC + c


def pairs(where):
    return [
        (rank_of(y, x, z, c), rank_of(*where(y, x, z, c)))
        for y in range(NY)
        for x in range(NX)
        for z in range(NZ)
        for c in range(NC)
    ]


def moved(value, where):
    return lax.ppermute(value, ALL, pairs(where))


def joined_rows(*parts):
    return jnp.concatenate(parts, axis=0)


def other_core(y, x, z, c):
    return (y, x, z, 1 - c)


def along_near(step):
    return lambda y, x, z, c: (y + step, x, z, c) if c == 0 else (y, x + step, z, c)


def along_far(step):
    return lambda y, x, z, c: (y, x + step, z, c) if c == 0 else (y + step, x, z, c)


def copy_for_each(shard, axis):
    copies = jnp.broadcast_to(shard, (lax.axis_size(axis), *shard.shape))
    return lax.all_to_all(copies, axis, split_axis=0, concat_axis=0, tiled=True)


def gathered(hidden):
    line = copy_for_each(hidden, "z").reshape(-1, hidden.shape[1])
    one = moved(line, along_near(-1))
    three = moved(line, along_near(1))
    two = moved(line, along_near(2))
    first = joined_rows(line, one)
    second = joined_rows(two, three)
    first_1 = moved(first, along_far(-1))
    second_3 = moved(second, along_far(1))
    second_1 = moved(second, along_far(-1))
    first_3 = moved(first, along_far(1))
    first_2 = moved(first_1, along_far(-1))
    second_2 = moved(second_3, along_far(1))
    return (first, second, first_1, second_3), (first_3, second_1, first_2, second_2)


EARLY = ((0, 0, 64), (1, 0, 64), (2, 0, 64), (3, 0, 64))
LATE = ((0, 0, 64), (1, 0, 64), (2, 0, 64), (3, 0, 64))


def piece_stats(heads, pieces, order, copies=(None, None)):
    depth = heads[0].shape[1]
    whole = jnp.concatenate([pieces[k][start:stop, :] for k, start, stop in order], axis=0)
    rows, notes = whole[:, :depth], whole[:, depth:]
    found = []
    for head, copy in zip(heads, copies):
        if copy is not None:
            copy.wait()
        for start in range(0, head.shape[0], CHUNK):
            stop = min(start + CHUNK, head.shape[0])
            logits = lax.dot_general(
                head[start:stop, :], rows, (((1,), (1,)), ((), ())), preferred_element_type=jnp.float32
            )
            peak = jnp.max(logits, axis=0, keepdims=True)
            shifted = logits - peak
            weight = jnp.exp(shifted)
            norm = jnp.sum(weight, axis=0, keepdims=True)
            tilt = jnp.sum(weight * shifted, axis=0, keepdims=True)
            found.append((peak, norm, tilt))
    peak = functools.reduce(jnp.maximum, [f[0] for f in found])
    norm, tilt = jnp.zeros_like(peak), jnp.zeros_like(peak)
    for p, n, t in found:
        shift = p - peak
        scale = jnp.exp(shift)
        norm += scale * n
        tilt += scale * (t + shift * n)
    picks = lax.broadcasted_iota(jnp.int32, (8, LANES), 0) == lax.broadcasted_iota(jnp.int32, (8, LANES), 1)
    marks = lax.dot_general(
        picks.astype(jnp.bfloat16), notes, (((1,), (1,)), ((), ())), preferred_element_type=jnp.float32
    )
    log_norm = jnp.log(norm)
    return jnp.concatenate([peak + log_norm, log_norm - tilt / norm, marks[:6]], axis=0)


def early_kernel(w0, w1, *refs):
    pieces, (out, v0, v1, sems) = refs[:-4], refs[-4:]
    copies = [pltpu.make_async_copy(w, v, sems.at[k]) for k, (w, v) in enumerate(((w0, v0), (w1, v1)))]
    for copy in copies:
        copy.start()
    out[...] = piece_stats((v0, v1), pieces, EARLY, copies)


def late_kernel(place, w0, w1, early, *refs):
    late = piece_stats((w0, w1), refs[:-1], LATE)
    out = refs[-1]
    far, near = place[0], place[1]
    low = lax.broadcasted_iota(jnp.int32, (8, LANES), 1) < LANES // 2
    a0, a1 = early[:, :LANES], early[:, LANES:]
    b0, b1 = late[:, :LANES], late[:, LANES:]
    turned = [a0, jnp.where(low, a1, b0), b1, jnp.where(low, b0, a1)]
    turned = [pltpu.roll(t, near * (LANES // 4), 1) for t in turned]
    for row in range(4):
        value = turned[row]
        for step in range(1, 4):
            value = jnp.where(far == step, turned[(row - step) % 4], value)
        for kind in range(4):
            out[4 * kind + row : 4 * kind + row + 1, :] = value[kind : kind + 1]


def joined(parts):
    level, spread = parts[:, :4], parts[:, 4:]
    top = jnp.max(level, axis=0)
    below = top[None] - level
    share = jnp.exp(-below)
    return top, jnp.sum(share, axis=0), jnp.sum(share * (below + spread), axis=0)


def in_vmem(*arrays):
    return [pltpu.with_memory_space_constraint(a, pltpu.VMEM) for a in arrays]


VMEM = pl.BlockSpec(memory_space=pltpu.VMEM)
ANY = pl.BlockSpec(memory_space=pl.ANY)


def cost(heads):
    rows, depth = 2 * heads[0].shape[0], heads[0].shape[1]
    return pl.CostEstimate(
        flops=4 * LANES * rows * depth,
        bytes_accessed=2 * (2 * LANES + rows) * depth,
        transcendentals=2 * LANES * rows,
    )


def early_stats(heads, pieces):
    return pl.pallas_call(
        early_kernel,
        out_shape=(
            jax.ShapeDtypeStruct((8, 2 * LANES), jnp.float32),
            *[pltpu.VMEM(h.shape, h.dtype) for h in heads],
        ),
        in_specs=[pl.BlockSpec(memory_space=pltpu.HBM)] * 2 + [VMEM] * len(pieces),
        out_specs=[VMEM] * 3,
        scratch_shapes=[pltpu.SemaphoreType.DMA((2,))],
        cost_estimate=cost(heads),
        compiler_params=pltpu.CompilerParams(vmem_limit_bytes=12 << 20),
    )(*[pltpu.with_memory_space_constraint(h, pltpu.HBM) for h in heads], *in_vmem(*pieces))


def late_stats(place, heads, early, pieces):
    return pl.pallas_call(
        late_kernel,
        out_shape=jax.ShapeDtypeStruct((16, LANES), jnp.float32),
        in_specs=[pl.BlockSpec(memory_space=pltpu.SMEM)] + [VMEM] * (3 + len(pieces)),
        out_specs=VMEM,
        cost_estimate=cost(heads),
        compiler_params=pltpu.CompilerParams(vmem_limit_bytes=12 << 20),
    )(place, *in_vmem(*heads, early, *pieces))


def per_device(hidden, unembed, loss_mask, seq_ids):
    y, x, z, c = (lax.axis_index(a) for a in ALL)
    near = jnp.where(c == 0, y, x)
    far = jnp.where(c == 0, x, y)
    heads = (unembed, moved(unembed, other_core))
    lane = lax.broadcasted_iota(jnp.int32, (hidden.shape[0], LANES), 1)
    notes = jnp.where(lane == 0, loss_mask[:, None], jnp.where(lane == 1, seq_ids[:, None], 0))
    early, late = gathered(jnp.concatenate([hidden, notes.astype(hidden.dtype)], axis=1))
    stats, *heads = early_stats(heads, early)
    stats = late_stats(jnp.stack([far, near]), heads, stats, late)
    kinds = jnp.arange(SEQS, dtype=jnp.int32)[:, None, None]
    member = (stats[8:12] > 0)[None] & (stats[12:16].astype(jnp.int32)[None] == kinds)
    member = member.astype(jnp.float32)
    counts = jnp.sum(member, axis=(1, 2))
    at = ((far * 4 + near) * NZ + z) * 4
    mine, member, counts, at = lax.optimization_barrier((stats[:8], member, counts, at))
    top, total, mixed = joined(copy_for_each(mine, "z"))
    log_total = jnp.log(total)
    both = jnp.concatenate([top + log_total, log_total + mixed / total], axis=0)
    top, total, mixed = joined(copy_for_each(both, ("y", "x")))
    entropy_rows = jnp.log(total) + mixed / total
    entropy = lax.dynamic_slice(entropy_rows.reshape(-1), (at,), (4,), allow_negative_indices=False)
    sums = jnp.sum(member * entropy_rows[None], axis=(1, 2))
    both = jnp.stack([sums, counts])
    both = both + moved(both, other_core)
    seq_mean = both[0] / jnp.maximum(both[1], 1.0)
    return (entropy, seq_mean)


def solution(mesh):
    split = Mesh(mesh.devices.reshape(NY, NX, NZ, NC), ALL)

    return jax.shard_map(
        per_device,
        mesh=split,
        in_specs=(P(ALL, None), P(ALL, None), P(ALL), P(ALL)),
        out_specs=(P(ALL), P()),
        check_vma=False,
    )
```

```python
import functools

import jax
import jax.numpy as jnp
from jax import lax
from jax.experimental import pallas as pl
from jax.experimental.pallas import tpu as pltpu
from jax.sharding import Mesh
from jax.sharding import PartitionSpec as P


SEQS = 8
NY, NX, NZ, NC = 4, 4, 8, 2
ALL = ("y", "x", "z", "c")
LANES = 128
CHUNK = 600


def rank_of(y, x, z, c):
    return (((y % NY) * NX + x % NX) * NZ + z % NZ) * NC + c


def pairs(where):
    return [
        (rank_of(y, x, z, c), rank_of(*where(y, x, z, c)))
        for y in range(NY)
        for x in range(NX)
        for z in range(NZ)
        for c in range(NC)
    ]


def moved(value, where):
    return lax.ppermute(value, ALL, pairs(where))


def joined_rows(*parts):
    return jnp.concatenate(parts, axis=0)


def other_core(y, x, z, c):
    return (y, x, z, 1 - c)


def along_near(step):
    return lambda y, x, z, c: (y + step, x, z, c) if c == 0 else (y, x + step, z, c)


def along_far(step):
    return lambda y, x, z, c: (y, x + step, z, c) if c == 0 else (y + step, x, z, c)


def copy_for_each(shard, axis):
    copies = jnp.broadcast_to(shard, (lax.axis_size(axis), *shard.shape))
    return lax.all_to_all(copies, axis, split_axis=0, concat_axis=0, tiled=True)


def gathered(hidden):
    line = copy_for_each(hidden, "z").reshape(-1, hidden.shape[1])
    one = moved(line, along_near(-1))
    three = moved(line, along_near(1))
    two = moved(line, along_near(2))
    first = joined_rows(line, one)
    second = joined_rows(two, three)
    first_1 = moved(first, along_far(-1))
    second_3 = moved(second, along_far(1))
    second_1 = moved(second, along_far(-1))
    first_3 = moved(first, along_far(1))
    first_2 = moved(first_1, along_far(-1))
    second_2 = moved(second_3, along_far(1))
    return (first, second, first_1, second_3), (first_3, second_1, first_2, second_2)


EARLY = ((0, 0, 64), (1, 0, 64), (2, 0, 64), (3, 0, 64))
LATE = ((0, 0, 64), (1, 0, 64), (2, 0, 64), (3, 0, 64))


def piece_stats(heads, pieces, order, copies=(None, None)):
    rows = jnp.concatenate([pieces[k][start:stop, :] for k, start, stop in order], axis=0)
    found = []
    for head, copy in zip(heads, copies):
        if copy is not None:
            copy.wait()
        for start in range(0, head.shape[0], CHUNK):
            stop = min(start + CHUNK, head.shape[0])
            logits = lax.dot_general(
                head[start:stop, :], rows, (((1,), (1,)), ((), ())), preferred_element_type=jnp.float32
            )
            peak = jnp.max(logits, axis=0, keepdims=True)
            shifted = logits - peak
            weight = jnp.exp(shifted)
            norm = jnp.sum(weight, axis=0, keepdims=True)
            tilt = jnp.sum(weight * shifted, axis=0, keepdims=True)
            found.append((peak, norm, tilt))
    peak = functools.reduce(jnp.maximum, [f[0] for f in found])
    norm, tilt = jnp.zeros_like(peak), jnp.zeros_like(peak)
    for p, n, t in found:
        shift = p - peak
        scale = jnp.exp(shift)
        norm += scale * n
        tilt += scale * (t + shift * n)
    log_norm = jnp.log(norm)
    return jnp.concatenate([peak + log_norm, log_norm - tilt / norm, jnp.zeros((6, rows.shape[0]), jnp.float32)], axis=0)


def early_kernel(w0, w1, *refs):
    pieces, (out, v0, v1, sems) = refs[:-4], refs[-4:]
    copies = [pltpu.make_async_copy(w, v, sems.at[k]) for k, (w, v) in enumerate(((w0, v0), (w1, v1)))]
    for copy in copies:
        copy.start()
    out[...] = piece_stats((v0, v1), pieces, EARLY, copies)


def late_kernel(place, masks, ids, w0, w1, early, *refs):
    late = piece_stats((w0, w1), refs[:-1], LATE)
    out = refs[-1]
    far, near, own = place[0], place[1], place[2]
    low = lax.broadcasted_iota(jnp.int32, (8, LANES), 1) < LANES // 2
    a0, a1 = early[:, :LANES], early[:, LANES:]
    b0, b1 = late[:, :LANES], late[:, LANES:]
    turned = [a0, jnp.where(low, a1, b0), b1, jnp.where(low, b0, a1)]
    turned = [pltpu.roll(t, near * (LANES // 4), 1) for t in turned]
    for row in range(4):
        value = turned[row]
        for step in range(1, 4):
            value = jnp.where(far == step, turned[(row - step) % 4], value)
        for kind in range(2):
            out[4 * kind + row : 4 * kind + row + 1, :] = value[kind : kind + 1]
    lane = lax.broadcasted_iota(jnp.int32, (4, LANES), 1)
    row = lax.broadcasted_iota(jnp.int32, (4, LANES), 0)
    for kind, notes in enumerate((masks, ids)):
        value = jnp.zeros((4, LANES), jnp.int32)
        for k in range(4):
            value = jnp.where((row == far) & (lane == own + k), notes[k], value)
        out[8 + 4 * kind : 12 + 4 * kind, :] = value.astype(jnp.float32)


def joined(parts):
    level, spread = parts[:, :4], parts[:, 4:8]
    top = jnp.max(level, axis=0)
    below = top[None] - level
    share = jnp.exp(-below)
    return top, jnp.sum(share, axis=0), jnp.sum(share * (below + spread), axis=0), jnp.sum(parts[:, 8:], axis=0)


def in_vmem(*arrays):
    return [pltpu.with_memory_space_constraint(a, pltpu.VMEM) for a in arrays]


VMEM = pl.BlockSpec(memory_space=pltpu.VMEM)
ANY = pl.BlockSpec(memory_space=pl.ANY)


def cost(heads):
    rows, depth = 2 * heads[0].shape[0], heads[0].shape[1]
    return pl.CostEstimate(
        flops=4 * LANES * rows * depth,
        bytes_accessed=2 * (2 * LANES + rows) * depth,
        transcendentals=2 * LANES * rows,
    )


def early_stats(heads, pieces):
    return pl.pallas_call(
        early_kernel,
        out_shape=(
            jax.ShapeDtypeStruct((8, 2 * LANES), jnp.float32),
            *[pltpu.VMEM(h.shape, h.dtype) for h in heads],
        ),
        in_specs=[pl.BlockSpec(memory_space=pltpu.HBM)] * 2 + [VMEM] * len(pieces),
        out_specs=[VMEM] * 3,
        scratch_shapes=[pltpu.SemaphoreType.DMA((2,))],
        cost_estimate=cost(heads),
        compiler_params=pltpu.CompilerParams(vmem_limit_bytes=12 << 20),
    )(*[pltpu.with_memory_space_constraint(h, pltpu.HBM) for h in heads], *in_vmem(*pieces))


def late_stats(places, heads, early, pieces):
    return pl.pallas_call(
        late_kernel,
        out_shape=jax.ShapeDtypeStruct((16, LANES), jnp.float32),
        in_specs=[pl.BlockSpec(memory_space=pltpu.SMEM)] * 3 + [VMEM] * (3 + len(pieces)),
        out_specs=VMEM,
        cost_estimate=cost(heads),
        compiler_params=pltpu.CompilerParams(vmem_limit_bytes=12 << 20),
    )(*places, *in_vmem(*heads, early, *pieces))


def per_device(hidden, unembed, loss_mask, seq_ids):
    y, x, z, c = (lax.axis_index(a) for a in ALL)
    near = jnp.where(c == 0, y, x)
    far = jnp.where(c == 0, x, y)
    heads = (unembed, moved(unembed, other_core))
    early, late = gathered(hidden)
    stats, *heads = early_stats(heads, early)
    own = near * (LANES // 4) + z * 4
    places = (jnp.stack([far, near, own]), loss_mask, seq_ids)
    stats = late_stats(places, heads, stats, late)
    stats, at = lax.optimization_barrier((stats, far * LANES + own))
    top, total, mixed, notes = joined(copy_for_each(stats, "z"))
    log_total = jnp.log(total)
    both = jnp.concatenate([top + log_total, log_total + mixed / total, notes], axis=0)
    top, total, mixed, notes = joined(copy_for_each(both, ("y", "x")))
    entropy_rows = jnp.log(total) + mixed / total
    entropy = lax.dynamic_slice(entropy_rows.reshape(-1), (at,), (4,), allow_negative_indices=False)
    kinds = jnp.arange(SEQS, dtype=jnp.int32)[:, None, None]
    member = (notes[:4] > 0)[None] & (notes[4:].astype(jnp.int32)[None] == kinds)
    member = member.astype(jnp.float32)
    counts = jnp.sum(member, axis=(1, 2))
    sums = jnp.sum(member * entropy_rows[None], axis=(1, 2))
    both = jnp.stack([sums, counts])
    both = both + moved(both, other_core)
    seq_mean = both[0] / jnp.maximum(both[1], 1.0)
    return (entropy, seq_mean)


def solution(mesh):
    split = Mesh(mesh.devices.reshape(NY, NX, NZ, NC), ALL)

    return jax.shard_map(
        per_device,
        mesh=split,
        in_specs=(P(ALL, None), P(ALL, None), P(ALL), P(ALL)),
        out_specs=(P(ALL), P()),
        check_vma=False,
    )
```
